32 devices in a mesh: shard: 8 (over z, y), model: 4 (over x, core).
Axes of the slice: x: 2, y: 2, z: 4, core: 2. Of those that a mesh axis runs over, the one named last changes fastest.
Arguments:
- w_query: bfloat16 [12288, 12288], P('shard', 'model'), may hold values from -0.078125 to 0.078125
- low_query: bfloat16 [12288, 16], P('shard'), may hold values from -0.0546875 to 0.0546875
- high_query: bfloat16 [16, 12288], P(None, 'model'), may hold values from -1.5 to 1.5
- w_key: bfloat16 [12288, 12288], P('shard', 'model'), may hold values from -0.078125 to 0.078125
- low_key: bfloat16 [12288, 16], P('shard'), may hold values from -0.0546875 to 0.0546875
- high_key: bfloat16 [16, 12288], P(None, 'model'), may hold values from -1.5 to 1.5
- w_value: bfloat16 [12288, 12288], P('shard', 'model'), may hold values from -0.078125 to 0.078125
- low_value: bfloat16 [12288, 16], P('shard'), may hold values from -0.0546875 to 0.0546875
- high_value: bfloat16 [16, 12288], P(None, 'model'), may hold values from -1.5 to 1.5
- norm_gain: float32 [12288], P('shard'), may hold values from 0.25 to 1.75
Outputs:
- final_query: bfloat16 [12288, 12288], P(None, ('model', 'shard'))
- final_key: bfloat16 [12288, 12288], P(None, ('model', 'shard'))
- final_value: bfloat16 [12288, 12288], P(None, ('model', 'shard'))
- scale_query: float32 [12288], P(('model', 'shard'))
- scale_key: float32 [12288], P(('model', 'shard'))
- scale_value: float32 [12288], P(('model', 'shard'))
The draws below stay inside these ranges and needn't reach their ends.
All inputs are finite; a program needn't handle non-finite values. Where the reference program divides by a largest or mean magnitude, that divisor is 1e-20 or more.
Results may differ from the reference program's by a relative error of at most 0.001.
Values may be sent and summed in bfloat16 or wider, within the bound.
A program may use at most 192 MiB of HBM per device.

```python
import jax
import jax.numpy as jnp

D_MODEL = 12288
Q_DIM = 12288
KV_DIM = 12288
RANK = 16


def with_spikes(values, key, source, target, blocks, factor):
    def block_of(dim):
        return (jnp.arange(values.shape[dim]) // (values.shape[dim] // blocks)).reshape((-1,) + (1,) * (values.ndim - 1 - dim))

    near = jax.random.permutation(key, blocks)[block_of(target)]
    second = (block_of(target) + blocks // 2) % blocks
    return jnp.where((block_of(source) == near) | (block_of(source) == second), factor * values, values)


def shard_levels(stream_key, extent, split, low, largest):
    gain, own = 1.0, jax.random.fold_in(stream_key, 6)
    for position, blocks in split:
        steps = jnp.exp(jax.random.uniform(jax.random.fold_in(own, position), (blocks,), jnp.float32, low / len(split), largest / len(split)))
        gain = gain * jnp.repeat(steps, extent[position] // blocks).reshape([-1 if axis == position else 1 for axis in range(len(extent))])
    return gain


def normal_values(stream_key, extent, width, reach, shards=(), dtype=jnp.bfloat16):
    entries = jax.random.normal(stream_key, extent, jnp.float32) * width
    if len(shards) > 0:
        entries = shard_levels(stream_key, extent, shards, -0.22, 0.18) * entries
    return jnp.clip(entries, min=-reach, max=reach).astype(dtype)


def heavy_noise(rng, extent, width, reach, cuts, heavy, kind=jnp.bfloat16):
    values = width * jax.random.normal(rng, extent, jnp.float32)
    if cuts:
        values = values * shard_levels(rng, extent, cuts, -0.22, 0.18)
    return jnp.clip(with_spikes(values, jax.random.fold_in(rng, 3), *heavy), -reach, reach).astype(kind)


def setup_inputs(seed: int = 0) -> dict:
    streams_of = jax.random.split(jax.random.key(seed), 11)
    w_query = heavy_noise(streams_of[0], (D_MODEL, Q_DIM), D_MODEL ** -0.5, 0.078125, ((0, 8), (1, 4)), (0, 1, 8, 2.0))
    low_query = normal_values(streams_of[1], (D_MODEL, RANK), D_MODEL ** -0.5, 0.0546875, ((0, 8),))
    high_query = normal_values(streams_of[2], (RANK, Q_DIM), RANK ** -0.5, 1.5, ((1, 4),))
    w_key = heavy_noise(streams_of[3], (D_MODEL, KV_DIM), D_MODEL ** -0.5, 0.078125, ((0, 8), (1, 4)), (0, 1, 8, 2.0))
    low_key = normal_values(streams_of[4], (D_MODEL, RANK), D_MODEL ** -0.5, 0.0546875, ((0, 8),))
    high_key = normal_values(streams_of[5], (RANK, KV_DIM), RANK ** -0.5, 1.5, ((1, 4),))
    w_value = heavy_noise(streams_of[6], (D_MODEL, KV_DIM), D_MODEL ** -0.5, 0.078125, ((0, 8), (1, 4)), (0, 1, 8, 2.0))
    low_value = normal_values(streams_of[7], (D_MODEL, RANK), D_MODEL ** -0.5, 0.0546875, ((0, 8),))
    high_value = normal_values(streams_of[8], (RANK, KV_DIM), RANK ** -0.5, 1.5, ((1, 4),))
    norm_gain = jnp.clip(1.0 + 0.15 * jax.random.normal(streams_of[9], (D_MODEL,), jnp.float32), 0.25, 1.75)
    return dict(w_query=w_query, low_query=low_query, high_query=high_query, w_key=w_key, low_key=low_key, high_key=high_key, w_value=w_value, low_value=low_value, high_value=high_value, norm_gain=norm_gain)


mix_rate = 1.0


def reference(w_query, low_query, high_query, w_key, low_key, high_key, w_value, low_value, high_value, norm_gain):
    result_query = w_query.astype(jnp.float32) + mix_rate * jnp.dot(low_query, high_query, preferred_element_type=jnp.float32)
    result_key = w_key.astype(jnp.float32) + mix_rate * jnp.dot(low_key, high_key, preferred_element_type=jnp.float32)
    result_value = w_value.astype(jnp.float32) + mix_rate * jnp.dot(low_value, high_value, preferred_element_type=jnp.float32)
    result_gained_query = result_query * norm_gain[:, None]
    result_gained_key = result_key * norm_gain[:, None]
    result_gained_value = result_value * norm_gain[:, None]
    scale_query = jnp.max(jnp.abs(result_gained_query), axis=0)
    final_query = (result_gained_query / scale_query).astype(jnp.bfloat16)
    scale_key = jnp.max(jnp.abs(result_gained_key), axis=0)
    final_key = (result_gained_key / scale_key).astype(jnp.bfloat16)
    scale_value = jnp.max(jnp.abs(result_gained_value), axis=0)
    final_value = (result_gained_value / scale_value).astype(jnp.bfloat16)
    return final_query, final_key, final_value, scale_query, scale_key, scale_value
```

```python
import functools

import jax
import jax.numpy as jnp
from jax import lax
from jax.experimental import pallas as pl
from jax.experimental.pallas import tpu as pltpu
from jax.sharding import PartitionSpec as P


mix_rate = 1.0
LANES = 128
PIECES = 16
SLOTS, AHEAD = 8, 4


def on_device_plain(
    w_query,
    low_query,
    high_query,
    w_key,
    low_key,
    high_key,
    w_value,
    low_value,
    high_value,
    norm_gain,
):
    def gained(w, low, high):
        delta = mix_rate * jnp.dot(low, high, preferred_element_type=jnp.float32)
        return (w.astype(jnp.float32) + delta) * norm_gain[:, None]

    gains = (
        gained(w_query, low_query, high_query),
        gained(w_key, low_key, high_key),
        gained(w_value, low_value, high_value),
    )
    scales = lax.pmax(tuple(jnp.max(jnp.abs(g), axis=0) for g in gains), "shard")
    finals = tuple(
        lax.all_to_all(
            (g / s).astype(jnp.bfloat16), "shard", split_axis=1, concat_axis=0, tiled=True
        )
        for g, s in zip(gains, scales)
    )
    width = finals[0].shape[1]
    start = lax.axis_index("shard") * width
    return finals + tuple(lax.dynamic_slice_in_dim(s, start, width) for s in scales)


def pack_kernel(jobs, *refs):
    out_ref, held, in_sem, out_sem = refs[-4:]

    def fetch(j):
        which, column, width, _, _ = jobs[j]
        w_ref = refs[which]
        return pltpu.make_async_copy(
            w_ref.at[:, pl.ds(column, width)],
            held.at[j % SLOTS, :, pl.ds(0, width)],
            in_sem.at[j % SLOTS],
        )

    def put(j):
        _, _, width, dest, at = jobs[j]
        rows = held.shape[1]
        return pltpu.make_async_copy(
            held.at[j % SLOTS, :, pl.ds(0, width)],
            out_ref.at[pl.ds(dest * rows, rows), pl.ds(at, width)],
            out_sem.at[j % SLOTS],
        )

    count = len(jobs)
    for j in range(count + AHEAD):
        if j < count:
            if j >= SLOTS:
                put(j - SLOTS).wait()
            fetch(j).start()
        if j >= AHEAD:
            fetch(j - AHEAD).wait()
            put(j - AHEAD).start()
    for j in range(max(0, count - SLOTS), count):
        put(j).wait()


def pack(weights, parts, n):
    rows, columns = weights[0].shape
    block = columns // n
    total = sum(width for _, _, width in parts)
    widest = max(width for _, _, width in parts)
    jobs = []
    for dest in range(n):
        at = 0
        for which, first, width in parts:
            jobs.append((which, dest * block + first, width, dest, at))
            at += width
    return pl.pallas_call(
        functools.partial(pack_kernel, tuple(jobs)),
        out_shape=jax.ShapeDtypeStruct((n * rows, total), weights[0].dtype),
        in_specs=[pl.BlockSpec(memory_space=pl.ANY)] * len(weights),
        out_specs=pl.BlockSpec(memory_space=pl.ANY),
        scratch_shapes=[
            pltpu.VMEM((SLOTS, rows, widest), weights[0].dtype),
            pltpu.SemaphoreType.DMA((SLOTS,)),
            pltpu.SemaphoreType.DMA((SLOTS,)),
        ],
        cost_estimate=pl.CostEstimate(
            flops=0, bytes_accessed=4 * n * rows * total, transcendentals=0
        ),
    )(*weights)


def merge_kernel(steps, raw_ref, left_ref, right_ref, *refs):
    out_ref, scale_ref, merged, peak = refs[-4:]
    step = pl.program_id(1)
    rows = raw_ref.shape[0]
    sub = 256 if rows % 256 == 0 else rows
    top = jnp.zeros((1, LANES), jnp.float32)
    for i in range(rows // sub):
        both = lax.dot_general(
            left_ref[:, i * sub : (i + 1) * sub],
            right_ref[...],
            (((0,), (0,)), ((), ())),
            preferred_element_type=jnp.float32,
        )
        delta, gain = both[:, :LANES], both[:, LANES:]
        base = raw_ref[i * sub : (i + 1) * sub, :].astype(jnp.float32)
        gained = (base + mix_rate * delta) * gain
        merged[pl.ds(pl.multiple_of(step * rows + i * sub, sub), sub), :] = gained
        top = jnp.maximum(top, jnp.max(jnp.abs(gained), axis=0, keepdims=True))
    so_far = jnp.where(step == 0, top, jnp.maximum(top, peak[0:1, :]))
    peak[0:1, :] = so_far

    @pl.when(step == steps - 1)
    def _():
        scale_ref[...] = so_far
        inverse = 1.0 / so_far

        @pl.loop(0, merged.shape[0] // sub)
        def _(i):
            here = pl.ds(pl.multiple_of(i * sub, sub), sub)
            out_ref[here, :] = (merged[here, :] * inverse).astype(out_ref.dtype)


def merge(raw, raw_tile, tiles, out_tile, columns, left, right, steps, earlier=()):
    height = raw.shape[0]
    rows, depth = height // steps, left.shape[0]
    return pl.pallas_call(
        functools.partial(merge_kernel, steps),
        grid=(tiles, steps),
        out_shape=(
            jax.ShapeDtypeStruct((height, columns), jnp.bfloat16),
            jax.ShapeDtypeStruct((1, columns), jnp.float32),
        ),
        in_specs=[
            pl.BlockSpec((rows, LANES), lambda t, s: (s, raw_tile + t)),
            pl.BlockSpec((depth, rows), lambda t, s: (0, s)),
            pl.BlockSpec((depth, 2 * LANES), lambda t, s: (0, out_tile + t)),
        ]
        + [pl.BlockSpec(memory_space=pl.ANY)] * len(earlier),
        out_specs=(
            pl.BlockSpec((height, LANES), lambda t, s: (0, out_tile + t)),
            pl.BlockSpec((1, LANES), lambda t, s: (0, out_tile + t)),
        ),
        scratch_shapes=[
            pltpu.VMEM((height, LANES), jnp.float32),
            pltpu.VMEM((8, LANES), jnp.float32),
        ],
        input_output_aliases={3 + i: i for i in range(len(earlier))},
        compiler_params=pltpu.CompilerParams(
            dimension_semantics=("arbitrary", "arbitrary"), vmem_limit_bytes=40 * 2**20
        ),
        cost_estimate=pl.CostEstimate(
            flops=4 * height * tiles * LANES * depth,
            bytes_accessed=4 * height * tiles * LANES,
            transcendentals=0,
        ),
    )(raw, left, right, *earlier)


def split_gain(gain):
    first = lax.reduce_precision(gain, 8, 7)
    second = lax.reduce_precision(gain - first, 8, 7)
    third = lax.reduce_precision(gain - first - second, 8, 7)
    return jnp.stack([first, second, third]).astype(jnp.bfloat16)


def gather_left(lows, norm_gain, n, m):
    rows, rank = lows[0].shape
    own = jnp.concatenate([low.T for low in lows] + [split_gain(norm_gain)], axis=0)
    count = len(lows) * rank
    lines = count + PIECES
    own = jnp.pad(own, ((0, lines - own.shape[0]), (0, 0)))
    part = rows // m
    mine = lax.dynamic_slice_in_dim(own, lax.axis_index("model") * part, part, axis=1)
    mine = lax.all_gather(mine, "shard")
    half = lines // 2
    every = jnp.concatenate(
        [lax.all_gather(mine[:, :half], "model"), lax.all_gather(mine[:, half:], "model")], axis=2
    )
    every = every.transpose(2, 1, 0, 3).reshape(lines, n * rows)
    return [
        jnp.concatenate([every[i * rank : (i + 1) * rank], every[count:]], axis=0)
        for i in range(len(lows))
    ]


def make_right(high, place, width):
    rank, tiles = high.shape[0], width // LANES
    mine = lax.dynamic_slice_in_dim(high, place * width, width, axis=1)
    mine = mine.reshape(rank, tiles, LANES)
    ones = (jnp.arange(PIECES) < 3).astype(high.dtype)[:, None, None]
    ones = jnp.broadcast_to(ones, (PIECES, tiles, LANES))
    top = jnp.concatenate([mine, jnp.zeros_like(mine)], axis=2)
    bottom = jnp.concatenate([jnp.zeros_like(ones), ones], axis=2)
    return jnp.concatenate([top, bottom], axis=0).reshape(rank + PIECES, 2 * width)


def on_device(
    n,
    m,
    w_query,
    low_query,
    high_query,
    w_key,
    low_key,
    high_key,
    w_value,
    low_value,
    high_value,
    norm_gain,
):
    width = w_query.shape[1] // n
    tiles = width // LANES
    place = lax.axis_index("shard")

    def exchange(packed):
        return lax.all_to_all(packed, "shard", split_axis=0, concat_axis=0, tiled=True)

    first = exchange(pack((w_query,), ((0, 0, LANES),), n))
    rest = width - LANES
    bulk = exchange(
        pack(
            (w_query, w_key, w_value),
            ((0, LANES, rest), (1, 0, width), (2, 0, rest)),
            n,
        ),
    )
    last = exchange(pack((w_value,), ((0, rest, LANES),), n))

    left_query, left_key, left_value = gather_left(
        (low_query, low_key, low_value), norm_gain, n, m
    )
    right_query = make_right(high_query, place, width)
    right_key = make_right(high_key, place, width)
    right_value = make_right(high_value, place, width)

    query = merge(first, 0, 1, 0, width, left_query, right_query, n)
    query = merge(bulk, 0, tiles - 1, 1, width, left_query, right_query, n, query)
    key = merge(bulk, tiles - 1, tiles, 0, width, left_key, right_key, n)
    value = merge(bulk, 2 * tiles - 1, tiles - 1, 0, width, left_value, right_value, n)
    value = merge(last, 0, 1, tiles - 1, width, left_value, right_value, n, value)
    finals, scales = zip(query, key, value)
    return finals + tuple(s.reshape(width) for s in scales)


def solution(mesh):
    n, m = mesh.shape["shard"], mesh.shape["model"]

    def chosen(*args):
        rows, columns = args[0].shape
        aligned = columns % (n * LANES) == 0 and columns // n >= 2 * LANES
        if aligned and rows % (m * LANES) == 0:
            return on_device(n, m, *args)
        return on_device_plain(*args)

    return jax.shard_map(
        chosen,
        mesh=mesh,
        in_specs=(
            P("shard", "model"),
            P("shard", None),
            P(None, "model"),
            P("shard", "model"),
            P("shard", None),
            P(None, "model"),
            P("shard", "model"),
            P("shard", None),
            P(None, "model"),
            P("shard"),
        ),
        out_specs=(
            P(None, ("model", "shard")),
            P(None, ("model", "shard")),
            P(None, ("model", "shard")),
            P(("model", "shard")),
            P(("model", "shard")),
            P(("model", "shard")),
        ),
        check_vma=False,
    )
```

```python
import functools

import jax
import jax.numpy as jnp
from jax import lax
from jax.experimental import pallas as pl
from jax.experimental.pallas import tpu as pltpu
from jax.sharding import PartitionSpec as P


mix_rate = 1.0
LANES = 128
PIECES = 16
SLOTS, AHEAD = 8, 4


def on_device_plain(
    w_query,
    low_query,
    high_query,
    w_key,
    low_key,
    high_key,
    w_value,
    low_value,
    high_value,
    norm_gain,
):
    def gained(w, low, high):
        delta = mix_rate * jnp.dot(low, high, preferred_element_type=jnp.float32)
        return (w.astype(jnp.float32) + delta) * norm_gain[:, None]

    gains = (
        gained(w_query, low_query, high_query),
        gained(w_key, low_key, high_key),
        gained(w_value, low_value, high_value),
    )
    scales = lax.pmax(tuple(jnp.max(jnp.abs(g), axis=0) for g in gains), "shard")
    finals = tuple(
        lax.all_to_all(
            (g / s).astype(jnp.bfloat16), "shard", split_axis=1, concat_axis=0, tiled=True
        )
        for g, s in zip(gains, scales)
    )
    width = finals[0].shape[1]
    start = lax.axis_index("shard") * width
    return finals + tuple(lax.dynamic_slice_in_dim(s, start, width) for s in scales)


def pack_kernel(jobs, *refs):
    out_ref, held, in_sem, out_sem = refs[-4:]

    def fetch(j):
        which, column, width, _, _ = jobs[j]
        w_ref = refs[which]
        return pltpu.make_async_copy(
            w_ref.at[:, pl.ds(column, width)],
            held.at[j % SLOTS, :, pl.ds(0, width)],
            in_sem.at[j % SLOTS],
        )

    def put(j):
        _, _, width, dest, at = jobs[j]
        rows = held.shape[1]
        return pltpu.make_async_copy(
            held.at[j % SLOTS, :, pl.ds(0, width)],
            out_ref.at[pl.ds(dest * rows, rows), pl.ds(at, width)],
            out_sem.at[j % SLOTS],
        )

    count = len(jobs)
    for j in range(count + AHEAD):
        if j < count:
            if j >= SLOTS:
                put(j - SLOTS).wait()
            fetch(j).start()
        if j >= AHEAD:
            fetch(j - AHEAD).wait()
            put(j - AHEAD).start()
    for j in range(max(0, count - SLOTS), count):
        put(j).wait()


def pack(weights, parts, n):
    rows, columns = weights[0].shape
    block = columns // n
    total = sum(width for _, _, width in parts)
    widest = max(width for _, _, width in parts)
    jobs = []
    for dest in range(n):
        at = 0
        for which, first, width in parts:
            jobs.append((which, dest * block + first, width, dest, at))
            at += width
    return pl.pallas_call(
        functools.partial(pack_kernel, tuple(jobs)),
        out_shape=jax.ShapeDtypeStruct((n * rows, total), weights[0].dtype),
        in_specs=[pl.BlockSpec(memory_space=pl.ANY)] * len(weights),
        out_specs=pl.BlockSpec(memory_space=pl.ANY),
        scratch_shapes=[
            pltpu.VMEM((SLOTS, rows, widest), weights[0].dtype),
            pltpu.SemaphoreType.DMA((SLOTS,)),
            pltpu.SemaphoreType.DMA((SLOTS,)),
        ],
        cost_estimate=pl.CostEstimate(
            flops=0, bytes_accessed=4 * n * rows * total, transcendentals=0
        ),
    )(*weights)


def merge_kernel(steps, raw_ref, left_ref, right_ref, *refs):
    out_ref, scale_ref, merged, peak = refs[-4:]
    step = pl.program_id(1)
    rows = raw_ref.shape[0]
    sub = 256 if rows % 256 == 0 else rows
    top = jnp.zeros((1, LANES), jnp.float32)
    for i in range(rows // sub):
        both = lax.dot_general(
            left_ref[:, i * sub : (i + 1) * sub],
            right_ref[...],
            (((0,), (0,)), ((), ())),
            preferred_element_type=jnp.float32,
        )
        delta, gain = both[:, :LANES], both[:, LANES:]
        base = raw_ref[i * sub : (i + 1) * sub, :].astype(jnp.float32)
        gained = (base + mix_rate * delta) * gain
        merged[pl.ds(pl.multiple_of(step * rows + i * sub, sub), sub), :] = gained
        top = jnp.maximum(top, jnp.max(jnp.abs(gained), axis=0, keepdims=True))
    so_far = jnp.where(step == 0, top, jnp.maximum(top, peak[0:1, :]))
    peak[0:1, :] = so_far

    @pl.when(step == steps - 1)
    def _():
        scale_ref[...] = so_far
        inverse = 1.0 / so_far

        @pl.loop(0, merged.shape[0] // sub)
        def _(i):
            here = pl.ds(pl.multiple_of(i * sub, sub), sub)
            out_ref[here, :] = (merged[here, :] * inverse).astype(out_ref.dtype)


def merge(raw, raw_tile, tiles, out_tile, columns, left, right, steps, earlier=()):
    height = raw.shape[0]
    rows, depth = height // steps, left.shape[0]
    return pl.pallas_call(
        functools.partial(merge_kernel, steps),
        grid=(tiles, steps),
        out_shape=(
            jax.ShapeDtypeStruct((height, columns), jnp.bfloat16),
            jax.ShapeDtypeStruct((1, columns), jnp.float32),
        ),
        in_specs=[
            pl.BlockSpec((rows, LANES), lambda t, s: (s, raw_tile + t)),
            pl.BlockSpec((depth, rows), lambda t, s: (0, s)),
            pl.BlockSpec((depth, 2 * LANES), lambda t, s: (0, out_tile + t)),
        ]
        + [pl.BlockSpec(memory_space=pl.ANY)] * len(earlier),
        out_specs=(
            pl.BlockSpec((height, LANES), lambda t, s: (0, out_tile + t)),
            pl.BlockSpec((1, LANES), lambda t, s: (0, out_tile + t)),
        ),
        scratch_shapes=[
            pltpu.VMEM((height, LANES), jnp.float32),
            pltpu.VMEM((8, LANES), jnp.float32),
        ],
        input_output_aliases={3 + i: i for i in range(len(earlier))},
        compiler_params=pltpu.CompilerParams(
            dimension_semantics=("arbitrary", "arbitrary"), vmem_limit_bytes=40 * 2**20
        ),
        cost_estimate=pl.CostEstimate(
            flops=4 * height * tiles * LANES * depth,
            bytes_accessed=4 * height * tiles * LANES,
            transcendentals=0,
        ),
    )(raw, left, right, *earlier)


def split_gain(gain):
    first = lax.reduce_precision(gain, 8, 7)
    second = lax.reduce_precision(gain - first, 8, 7)
    third = lax.reduce_precision(gain - first - second, 8, 7)
    return jnp.stack([first, second, third]).astype(jnp.bfloat16)


def gather_left(lows, norm_gain, n, m):
    rows, rank = lows[0].shape
    own = jnp.concatenate([low.T for low in lows] + [split_gain(norm_gain)], axis=0)
    count = len(lows) * rank
    lines = count + PIECES
    own = jnp.pad(own, ((0, lines - own.shape[0]), (0, 0)))
    part = rows // m
    mine = lax.dynamic_slice_in_dim(own, lax.axis_index("model") * part, part, axis=1)
    mine = lax.all_gather(mine, "shard")
    half = lines // 2
    halves = mine[:, :half], mine[:, half:]
    halves = [lax.all_gather(one, "model") for one in halves]
    every = jnp.concatenate(halves, axis=2)
    every = every.transpose(2, 1, 0, 3).reshape(lines, n * rows)
    return [
        jnp.concatenate([every[i * rank : (i + 1) * rank], every[count:]], axis=0)
        for i in range(len(lows))
    ]


def make_right(high, place, width):
    rank, tiles = high.shape[0], width // LANES
    mine = lax.dynamic_slice_in_dim(high, place * width, width, axis=1)
    mine = mine.reshape(rank, tiles, LANES)
    ones = (jnp.arange(PIECES) < 3).astype(high.dtype)[:, None, None]
    ones = jnp.broadcast_to(ones, (PIECES, tiles, LANES))
    top = jnp.concatenate([mine, jnp.zeros_like(mine)], axis=2)
    bottom = jnp.concatenate([jnp.zeros_like(ones), ones], axis=2)
    return jnp.concatenate([top, bottom], axis=0).reshape(rank + PIECES, 2 * width)


def on_device(
    n,
    m,
    w_query,
    low_query,
    high_query,
    w_key,
    low_key,
    high_key,
    w_value,
    low_value,
    high_value,
    norm_gain,
):
    width = w_query.shape[1] // n
    tiles = width // LANES
    place = lax.axis_index("shard")

    def exchange(packed):
        return lax.all_to_all(packed, "shard", split_axis=0, concat_axis=0, tiled=True)

    first = exchange(pack((w_query,), ((0, 0, LANES),), n))
    rest = width - LANES
    packed = pack(
        (w_query, w_key, w_value),
        ((0, LANES, rest), (1, 0, width), (2, 0, rest)),
        n,
    )
    bulk = exchange(packed)
    last = exchange(pack((w_value,), ((0, rest, LANES),), n))

    left_query, left_key, left_value = gather_left(
        (low_query, low_key, low_value), norm_gain, n, m
    )
    right_query = make_right(high_query, place, width)
    right_key = make_right(high_key, place, width)
    right_value = make_right(high_value, place, width)

    query = merge(first, 0, 1, 0, width, left_query, right_query, n)
    query = merge(bulk, 0, tiles - 1, 1, width, left_query, right_query, n, query)
    key = merge(bulk, tiles - 1, tiles, 0, width, left_key, right_key, n)
    value = merge(bulk, 2 * tiles - 1, tiles - 1, 0, width, left_value, right_value, n)
    value = merge(last, 0, 1, tiles - 1, width, left_value, right_value, n, value)
    finals, scales = zip(query, key, value)
    return finals + tuple(s.reshape(width) for s in scales)


def solution(mesh):
    n, m = mesh.shape["shard"], mesh.shape["model"]

    def chosen(*args):
        rows, columns = args[0].shape
        aligned = columns % (n * LANES) == 0 and columns // n >= 2 * LANES
        if aligned and rows % (m * LANES) == 0:
            return on_device(n, m, *args)
        return on_device_plain(*args)

    return jax.shard_map(
        chosen,
        mesh=mesh,
        in_specs=(
            P("shard", "model"),
            P("shard", None),
            P(None, "model"),
            P("shard", "model"),
            P("shard", None),
            P(None, "model"),
            P("shard", "model"),
            P("shard", None),
            P(None, "model"),
            P("shard"),
        ),
        out_specs=(
            P(None, ("model", "shard")),
            P(None, ("model", "shard")),
            P(None, ("model", "shard")),
            P(("model", "shard")),
            P(("model", "shard")),
            P(("model", "shard")),
        ),
        check_vma=False,
    )
```
